32 devices in a mesh: hw: 8 (over y, x, core), head: 4 (over z).
Axes of the slice: x: 2, y: 2, z: 4, core: 2. Of those that a mesh axis runs over, the one named last changes fastest.
Arguments:
- latents: bfloat16 [8, 8, 8, 8, 5120], P('hw'), may hold values from -6 to 6
- query_weight: bfloat16 [5120, 2560], P('hw', 'head'), may hold values from -0.125 to 0.125
- key_weight: bfloat16 [5120, 2560], P('hw', 'head'), may hold values from -0.125 to 0.125
- value_weight: bfloat16 [5120, 2560], P('hw', 'head'), may hold values from -0.078125 to 0.078125
- output_weight: bfloat16 [2560, 5120], P('hw', 'head'), may hold values from -0.5 to 0.5
- query_gain: float32 [2560], P('head'), may hold values from 0.3 to 9
- key_gain: float32 [2560], P('head'), may hold values from 0.3 to 9
- frame_index: int32 [8], replicated, may hold values from 0 to 94, as said below
- row_index: int32 [32], replicated, may hold values from 0 to 286, as said below
- column_index: int32 [16], replicated, may hold values from 0 to 158, as said below
Outputs:
- attention_out: bfloat16 [8, 8, 8, 8, 5120], P('hw', None, None, None, 'head')
The draws below stay inside these ranges and needn't reach their ends.
Inputs may be any that keep to these rules, and one draw needn't show every extreme that they name: `frame_index`: strictly increasing. `row_index`: strictly increasing. `column_index`: strictly increasing.
All inputs are finite; a program needn't handle non-finite values.
Results may differ from the reference program's by a relative error of at most 0.0075.
The reference program's roundings to bfloat16 on the way count: a program that leaves them out, or rounds other values in their place, can miss the bound.
Values may be sent and summed in bfloat16 or wider, within the bound.
A program may use at most 128 MiB of HBM per device.

```python
import math
import jax
import jax.numpy as jnp
from jax import lax

D = 5120
HEADS = 20
HD = 128
WT = 4
DEV_ROWS = 4
FRAMES = 8
BS = 8
GRID_W = 2
BLOCKS = 8
HH = 32
WW = 16


def gain_values(key, salt):
    subkey = jax.random.fold_in(key, salt)
    return jnp.exp(jax.random.uniform(subkey, (HEADS * HD,), jnp.float32, -1.2, 1.2))


def position_values(key, salt, count):
    subkey = jax.random.fold_in(key, salt)
    top_stride = 30 // count + 8
    strides = jax.random.randint(subkey, (count,), 1, top_stride + 1, dtype=jnp.int32)
    total = jnp.sum(strides)
    most = jnp.int32(30 + 8 * count)
    return (most - (total - jnp.cumsum(strides))).astype(jnp.int32)


def draw_query_gain(key, part):
    return gain_values(key, 11)


def draw_key_gain(key, part):
    return gain_values(key, 12)


def draw_frame_index(key, part):
    return position_values(key, 21, FRAMES)


def draw_row_index(key, part):
    return position_values(key, 22, HH)


def draw_column_index(key, part):
    return position_values(key, 23, WW)


def strengthened(entries, key, source, target, blocks, factor):
    def block_of(position):
        return (jnp.arange(entries.shape[position]) // (entries.shape[position] // blocks)).reshape((-1,) + (1,) * (entries.ndim - 1 - position))

    near = jax.random.permutation(key, blocks)[block_of(target)]
    second = (block_of(target) + blocks // 2) % blocks
    return jnp.where((block_of(source) == near) | (block_of(source) == second), factor * entries, entries)


def level_of(stream_key, extent, shards, low, largest):
    def one(axis_at, parts):
        steps = jax.random.uniform(jax.random.fold_in(jax.random.fold_in(stream_key, 6), axis_at), (parts,), jnp.float32, low / len(shards), largest / len(shards))
        return jnp.repeat(jnp.exp(steps), extent[axis_at] // parts).reshape((-1,) + (1,) * (len(extent) - axis_at - 1))

    factor_of = one(*shards[0])
    for cut in shards[1:]:
        factor_of = factor_of * one(*cut)
    return factor_of


def normal_values(own_key, extent, deviation, reach, split=(), held_as=jnp.bfloat16):
    values = jax.random.normal(own_key, extent, jnp.float32) * deviation
    if len(split) > 0:
        values = level_of(own_key, extent, split, -0.22, 0.18) * values
    return jnp.clip(values, min=-reach, max=reach).astype(held_as)


def heavy_noise(rng, extent, deviation, most, shards, heavy, kind=jnp.bfloat16):
    values = deviation * jax.random.normal(rng, extent, jnp.float32)
    if shards:
        values = values * level_of(rng, extent, shards, -0.22, 0.18)
    return jnp.clip(strengthened(values, jax.random.fold_in(rng, 3), *heavy), -most, most).astype(kind)


def setup_inputs(seed: int = 0) -> dict:
    seeds = jax.random.split(jax.random.key(seed), 11)
    return {
        "latents": normal_values(seeds[0], (BLOCKS, FRAMES, BS, BS, D), 1.0, 6.0, ((0, 8),)),
        "query_weight": heavy_noise(seeds[1], (D, HEADS * HD), D ** -0.5, 0.125, ((0, 8), (1, 4)), (0, 1, 8, 2.0)),
        "key_weight": heavy_noise(seeds[2], (D, HEADS * HD), D ** -0.5, 0.125, ((0, 8), (1, 4)), (0, 1, 8, 2.0)),
        "value_weight": normal_values(seeds[3], (D, HEADS * HD), D ** -0.5, 0.078125, ((0, 8), (1, 4))),
        "output_weight": normal_values(seeds[4], (HEADS * HD, D), (HEADS * HD // 16) ** -0.5, 0.5, ((0, 8), (1, 4))),
        "query_gain": draw_query_gain(jax.random.fold_in(seeds[10], 71), 0),
        "key_gain": draw_key_gain(jax.random.fold_in(seeds[10], 71), 0),
        "frame_index": draw_frame_index(jax.random.fold_in(seeds[10], 71), 0),
        "row_index": draw_row_index(jax.random.fold_in(seeds[10], 71), 0),
        "column_index": draw_column_index(jax.random.fold_in(seeds[10], 71), 0),
    }


NORM_EPS = 0.5

def freq_table(count):
    ratios = jnp.arange(count, dtype=jnp.float32) / count
    return jnp.float32(10000.0) ** (-ratios)

def rope_angles(frame_index, row_index, column_index, head_dim):
    side_pairs = head_dim // 6
    frame_pairs = head_dim // 2 - 2 * side_pairs
    frame_part = frame_index.astype(jnp.float32)[:, None] * freq_table(frame_pairs)[None, :]
    row_part = row_index.astype(jnp.float32)[:, None] * freq_table(side_pairs)[None, :]
    column_part = column_index.astype(jnp.float32)[:, None] * freq_table(side_pairs)[None, :]
    frames, rows, columns = (frame_part.shape[0], row_part.shape[0], column_part.shape[0])
    return jnp.concatenate([jnp.broadcast_to(frame_part[:, None, None, :], (frames, rows, columns, frame_pairs)), jnp.broadcast_to(row_part[None, :, None, :], (frames, rows, columns, side_pairs)), jnp.broadcast_to(column_part[None, None, :, :], (frames, rows, columns, side_pairs))], axis=-1)

def pair_turn(head_dim):
    source = jnp.arange(head_dim)[:, None]
    target = jnp.arange(head_dim)[None, :]
    plus = ((target % 2 == 1) & (source == target - 1)).astype(jnp.float32)
    minus = ((target % 2 == 0) & (source == target + 1)).astype(jnp.float32)
    return plus - minus

def rotate(features, angle, heads_here, head_dim):
    frames, rows, columns = (angle.shape[0], angle.shape[1], angle.shape[2])
    cosine = jnp.repeat(jnp.cos(angle), 2, axis=-1)[:, :, :, None, :]
    sine = jnp.repeat(jnp.sin(angle), 2, axis=-1)[:, :, :, None, :]
    shaped = features.reshape(frames, rows, columns, heads_here, head_dim)
    turned = jnp.dot(shaped.reshape(-1, head_dim), pair_turn(head_dim), precision=lax.Precision.HIGHEST).reshape(shaped.shape)
    rotated = shaped * cosine + turned * sine
    return rotated.astype(jnp.bfloat16).reshape(frames, rows, columns, heads_here * head_dim)

def soft_weights(scores):
    top = lax.optimization_barrier(jnp.max(scores, axis=-1, keepdims=True))
    raised = jnp.exp(scores - top)
    return (raised / lax.optimization_barrier(jnp.sum(raised, axis=-1, keepdims=True))).astype(jnp.bfloat16)

def window_attend(queries, keys, values, first_row, first_column, total_rows, total_columns, heads_here, head_dim):
    frames, rows, columns, width = queries.shape
    across = rows // WT
    along = columns // WT
    area = WT * WT
    scale = 1.0 / math.sqrt(head_dim)

    def tiles(array, extra):
        shaped = array.reshape(frames, across + extra, WT, along + extra, WT, heads_here, head_dim)
        return shaped.transpose(0, 1, 3, 2, 4, 5, 6).reshape(frames, across + extra, along + extra, area, heads_here, head_dim)
    query_tiles = tiles(queries, 0)
    key_tiles = tiles(keys, 2)
    value_tiles = tiles(values, 2)
    offsets = [(down, right) for down in range(3) for right in range(3)]
    key_window = jnp.concatenate([key_tiles[:, down:down + across, right:right + along] for down, right in offsets], axis=3)
    value_window = jnp.concatenate([value_tiles[:, down:down + across, right:right + along] for down, right in offsets], axis=3)
    tile_rows = first_row + jnp.arange(across)
    tile_columns = first_column + jnp.arange(along)
    inside = []
    for down, right in offsets:
        row_ok = (tile_rows + down - 1 >= 0) & (tile_rows + down - 1 < total_rows)
        column_ok = (tile_columns + right - 1 >= 0) & (tile_columns + right - 1 < total_columns)
        inside.append(row_ok[:, None] & column_ok[None, :])
    allowed = jnp.repeat(jnp.stack(inside, axis=-1), area, axis=-1)
    scores = jnp.einsum('fabqhd,fabkhd->fabhqk', query_tiles.astype(jnp.float32), key_window.astype(jnp.float32)) * scale
    scores = jnp.where(allowed[None, :, :, None, None, :], scores, -jnp.inf)
    weights = soft_weights(scores)
    mixed = jnp.einsum('fabhqk,fabkhd->fabqhd', weights.astype(jnp.float32), value_window.astype(jnp.float32)).astype(jnp.bfloat16)
    mixed = mixed.reshape(frames, across, along, WT, WT, heads_here, head_dim)
    return mixed.transpose(0, 1, 3, 2, 4, 5, 6).reshape(frames, rows, columns, width)

def frame_attend(queries, keys, values, heads_here, head_dim):
    frames = queries.shape[0]
    scale = 1.0 / math.sqrt(head_dim)
    query_rows = queries.reshape(frames, -1, heads_here, head_dim).astype(jnp.float32)
    key_rows = keys.reshape(frames, -1, heads_here, head_dim).astype(jnp.float32)
    value_rows = values.reshape(frames, -1, heads_here, head_dim).astype(jnp.float32)
    scores = jnp.einsum('fphd,gphd->phfg', query_rows, key_rows) * scale
    weights = soft_weights(scores)
    mixed = jnp.einsum('phfg,gphd->fphd', weights.astype(jnp.float32), value_rows).astype(jnp.bfloat16)
    return mixed.reshape(queries.shape)

def to_grid(tokens, frames, side):
    width = tokens.shape[-1]
    shaped = tokens.reshape(DEV_ROWS, GRID_W, frames, side, side, width)
    return shaped.transpose(2, 0, 3, 1, 4, 5).reshape(frames, DEV_ROWS * side, GRID_W * side, width)

def from_grid(grid, side):
    frames, width = (grid.shape[0], grid.shape[-1])
    shaped = grid.reshape(frames, DEV_ROWS, side, GRID_W, side, width)
    return shaped.transpose(1, 3, 0, 2, 4, 5).reshape(-1, width)

def reference(latents, query_weight, key_weight, value_weight, output_weight, query_gain, key_gain, frame_index, row_index, column_index):
    frames, side, width = (latents.shape[1], latents.shape[2], latents.shape[4])
    full_width = query_weight.shape[1]
    heads_all = full_width // HD
    tokens = latents.reshape(-1, width)
    query_lin = jnp.dot(tokens, query_weight, preferred_element_type=jnp.float32)
    key_lin = jnp.dot(tokens, key_weight, preferred_element_type=jnp.float32)
    values = jnp.dot(tokens, value_weight, preferred_element_type=jnp.float32).astype(jnp.bfloat16)
    query_norm = query_lin * lax.rsqrt(lax.optimization_barrier(jnp.sum(query_lin * query_lin, axis=1)) / full_width + NORM_EPS)[:, None] * query_gain
    key_norm = key_lin * lax.rsqrt(lax.optimization_barrier(jnp.sum(key_lin * key_lin, axis=1)) / full_width + NORM_EPS)[:, None] * key_gain
    angle = rope_angles(frame_index, row_index, column_index, HD)
    queries = rotate(to_grid(query_norm, frames, side), angle, heads_all, HD)
    keys = rotate(to_grid(key_norm, frames, side), angle, heads_all, HD)
    values_grid = to_grid(values, frames, side)
    margin = ((0, 0), (WT, WT), (WT, WT), (0, 0))
    keys_padded = jnp.pad(keys, margin)
    values_padded = jnp.pad(values_grid, margin)
    tile_rows = queries.shape[1] // WT
    tile_columns = queries.shape[2] // WT

    def one_frame(items):
        query_frame, key_frame, value_frame = items
        return window_attend(query_frame[None], key_frame[None], value_frame[None], 0, 0, tile_rows, tile_columns, heads_all, HD)[0]
    spatial = lax.map(one_frame, (queries, keys_padded, values_padded))
    mixed = frame_attend(queries, keys, spatial, heads_all, HD)
    result = jnp.dot(from_grid(mixed, side), output_weight, preferred_element_type=jnp.float32).astype(jnp.bfloat16)
    return result.reshape(latents.shape)
```

```python
import functools
import math

import jax
import jax.numpy as jnp
from jax import lax
from jax.experimental import pallas as pl
from jax.experimental.pallas import tpu as pltpu
from jax.sharding import PartitionSpec as P

HEADS = 20
HD = 128
WT = 4
DEV_ROWS = 4


NORM_EPS = 0.5


def from_behind(value, axis, steps):
    count = lax.axis_size(axis)
    initial, last = (max(0, -steps), min(count, count - steps))
    return lax.ppermute(value, axis, [(source, source + steps) for source in range(initial, last)])


def freq_table(count):
    ratios = jnp.arange(count, dtype=jnp.float32) / count
    return jnp.float32(10000.0) ** (-ratios)


def rope_angles(frame_index, row_index, column_index, head_dim):
    side_pairs = head_dim // 6
    frame_pairs = head_dim // 2 - 2 * side_pairs
    frame_part = frame_index.astype(jnp.float32)[:, None] * freq_table(frame_pairs)[None, :]
    row_part = row_index.astype(jnp.float32)[:, None] * freq_table(side_pairs)[None, :]
    column_part = column_index.astype(jnp.float32)[:, None] * freq_table(side_pairs)[None, :]
    frames, rows, columns = (frame_part.shape[0], row_part.shape[0], column_part.shape[0])
    return jnp.concatenate(
        [
            jnp.broadcast_to(frame_part[:, None, None, :], (frames, rows, columns, frame_pairs)),
            jnp.broadcast_to(row_part[None, :, None, :], (frames, rows, columns, side_pairs)),
            jnp.broadcast_to(column_part[None, None, :, :], (frames, rows, columns, side_pairs)),
        ],
        axis=-1,
    )


def pair_turn(head_dim):
    source = jnp.arange(head_dim)[:, None]
    target = jnp.arange(head_dim)[None, :]
    plus = ((target % 2 == 1) & (source == target - 1)).astype(jnp.float32)
    minus = ((target % 2 == 0) & (source == target + 1)).astype(jnp.float32)
    return plus - minus


def rotate(features, angle, heads_here, head_dim):
    frames, rows, columns = (angle.shape[0], angle.shape[1], angle.shape[2])
    cosine = jnp.repeat(jnp.cos(angle), 2, axis=-1)[:, :, :, None, :]
    sine = jnp.repeat(jnp.sin(angle), 2, axis=-1)[:, :, :, None, :]
    shaped = features.reshape(frames, rows, columns, heads_here, head_dim)
    turned = jnp.dot(
        shaped.reshape(-1, head_dim), pair_turn(head_dim), precision=lax.Precision.HIGHEST
    ).reshape(shaped.shape)
    rotated = shaped * cosine + turned * sine
    return rotated.astype(jnp.bfloat16).reshape(frames, rows, columns, heads_here * head_dim)


def soft_weights(scores):
    top = jnp.max(scores, axis=-1, keepdims=True)
    raised = jnp.exp(scores - top)
    return (raised / jnp.sum(raised, axis=-1, keepdims=True)).astype(jnp.bfloat16)


def window_attend(
    queries, keys, values, first_row, first_column, total_rows, total_columns, heads_here, head_dim
):
    frames, rows, columns, width = queries.shape
    across = rows // WT
    along = columns // WT
    area = WT * WT
    scale = 1.0 / math.sqrt(head_dim)

    def tiles(array, extra):
        shaped = array.reshape(frames, across + extra, WT, along + extra, WT, heads_here, head_dim)
        return shaped.transpose(0, 1, 3, 2, 4, 5, 6).reshape(
            frames, across + extra, along + extra, area, heads_here, head_dim
        )

    query_tiles = tiles(queries, 0)
    key_tiles = tiles(keys, 2)
    value_tiles = tiles(values, 2)
    offsets = [(down, right) for down in range(3) for right in range(3)]
    key_window = jnp.concatenate(
        [key_tiles[:, down : down + across, right : right + along] for down, right in offsets],
        axis=3,
    )
    value_window = jnp.concatenate(
        [value_tiles[:, down : down + across, right : right + along] for down, right in offsets],
        axis=3,
    )
    tile_rows = first_row + jnp.arange(across)
    tile_columns = first_column + jnp.arange(along)
    inside = []
    for down, right in offsets:
        row_ok = (tile_rows + down - 1 >= 0) & (tile_rows + down - 1 < total_rows)
        column_ok = (tile_columns + right - 1 >= 0) & (tile_columns + right - 1 < total_columns)
        inside.append(row_ok[:, None] & column_ok[None, :])
    allowed = jnp.repeat(jnp.stack(inside, axis=-1), area, axis=-1)
    scores = (
        jnp.einsum(
            "fabqhd,fabkhd->fabhqk", query_tiles, key_window, preferred_element_type=jnp.float32
        )
        * scale
    )
    scores = jnp.where(allowed[None, :, :, None, None, :], scores, -jnp.inf)
    weights = soft_weights(scores)
    mixed = jnp.einsum(
        "fabhqk,fabkhd->fabqhd", weights, value_window, preferred_element_type=jnp.float32
    ).astype(jnp.bfloat16)
    mixed = mixed.reshape(frames, across, along, WT, WT, heads_here, head_dim)
    return mixed.transpose(0, 1, 3, 2, 4, 5, 6).reshape(frames, rows, columns, width)


def frame_attend(queries, keys, values, heads_here, head_dim):
    frames = queries.shape[0]
    scale = 1.0 / math.sqrt(head_dim)
    query_rows = queries.reshape(frames, -1, heads_here, head_dim)
    key_rows = keys.reshape(frames, -1, heads_here, head_dim)
    value_rows = values.reshape(frames, -1, heads_here, head_dim)
    scores = (
        jnp.einsum("fphd,gphd->phfg", query_rows, key_rows, preferred_element_type=jnp.float32)
        * scale
    )
    weights = soft_weights(scores)
    mixed = jnp.einsum(
        "phfg,gphd->fphd", weights, value_rows, preferred_element_type=jnp.float32
    ).astype(jnp.bfloat16)
    return mixed.reshape(queries.shape)


def region(stack, down, right, edge):
    rows = stack.shape[2]
    columns = stack.shape[3]
    row_start, row_stop = (rows - edge, rows) if down < 0 else (0, edge) if down > 0 else (0, rows)
    column_start, column_stop = (
        (columns - edge, columns) if right < 0 else (0, edge) if right > 0 else (0, columns)
    )
    return stack[:, :, row_start:row_stop, column_start:column_stop]


CUBE = 8


class Cube:
    def __init__(self, stride):
        me = lax.axis_index("hw")
        within = lax.rem(me, stride) if stride > 1 else 0
        place = lax.div(me, stride) if stride > 1 else me
        core = lax.rem(place, 2)
        x = lax.rem(lax.div(place, 2), 2)
        y = lax.div(place, 4)
        self.place = place
        self.other = [place + 1 - 2 * core, place + 2 - 4 * x, place + 4 - 8 * y]
        self.diagonal = place + 2 - 4 * x + 4 - 8 * y
        self.devices = [{"hw": other * stride + within} for other in self.other]
        self.chip = lax.div(place, 2)
        self.chips = [
            self.chip,
            self.chip + 1 - 2 * x,
            self.chip + 2 - 4 * y,
            self.chip + 3 - 2 * x - 4 * y,
        ]

    def barrier(self):
        semaphore = pltpu.get_barrier_semaphore()
        for device in self.devices:
            pl.semaphore_signal(semaphore, inc=1, device_id=device, device_id_type=pl.DeviceIdType.MESH)
        pl.semaphore_wait(semaphore, len(self.devices))


class Exchange:
    def __init__(self, cube, held, send, receive, rows):
        core_place, x_place, y_place = cube.other
        half = rows // 2

        def part(place, low, size):
            start = pl.multiple_of(lax.rem(place, 2) * rows + low, 16)
            return held.at[lax.div(place, 2), pl.ds(start, size)]

        def copy(at, place, low, size, partner):
            ref = part(place, low, size)
            return pltpu.make_async_remote_copy(
                src_ref=ref,
                dst_ref=ref,
                send_sem=send.at[at],
                recv_sem=receive.at[at],
                device_id=cube.devices[partner],
                device_id_type=pl.DeviceIdType.MESH,
            )

        self.own = part(cube.place, 0, rows)
        self.copies = [
            copy(0, cube.place, 0, rows, 1),
            copy(1, cube.place, 0, rows, 2),
            copy(2, cube.place, 0, rows, 0),
            copy(3, x_place, 0, rows, 0),
            copy(4, y_place, 0, rows, 0),
            copy(5, x_place, 0, half, 2),
            copy(6, y_place, half, half, 1),
            copy(7, cube.diagonal, 0, half, 0),
            copy(8, cube.diagonal, half, half, 0),
        ]

    def start(self, *which):
        for at in which:
            self.copies[at].start()

    def arrived(self, *which):
        for at in which:
            self.copies[at].wait_recv()

    def sent(self):
        for one in self.copies:
            one.wait_send()


def project_kernel(
    stride, tokens_hbm, query_hbm, key_hbm, value_hbm, output_hbm,
    query_ref, key_ref, value_ref, output_all,
    tokens, held, value_sum, local, send, receive,
):
    cube = Cube(stride)
    rows = query_hbm.shape[0]
    depth = 2 * rows
    weights = [
        Exchange(cube, held.at[at], send.at[at], receive.at[at], rows) for at in range(3)
    ] + [Exchange(cube, output_all, send.at[3], receive.at[3], output_hbm.shape[0])]
    loads = [
        pltpu.make_async_copy(source, weight.own, local.at[at])
        for at, (source, weight) in enumerate(
            zip((query_hbm, key_hbm, value_hbm, output_hbm), weights)
        )
    ]
    fetch = pltpu.make_async_copy(tokens_hbm, tokens, local.at[4])
    for load in loads:
        load.start()
    fetch.start()
    cube.barrier()
    query, key, value, output = weights
    loads[0].wait()
    query.start(2, 0, 1)
    loads[1].wait()
    key.start(2, 0, 1)
    sums = [query_ref, key_ref, value_sum]
    block = tokens.shape[0] // 2

    def multiply(at, lane):
        chip = cube.chips[lane]

        @pl.loop(0, 2)
        def _(step):
            here = pl.ds(pl.multiple_of(step * block, block), block)
            product = jnp.dot(
                tokens[here, pl.ds(pl.multiple_of(chip * depth, 128), depth)],
                held[at, chip],
                preferred_element_type=jnp.float32,
            )
            if lane == 0:
                sums[at][here, :] = product
            else:
                sums[at][here, :] += product

    def near(weight):
        weight.arrived(0)
        weight.start(5, 3)
        weight.arrived(1)
        weight.start(6, 4)

    def far(weight):
        weight.arrived(5)
        weight.start(7)
        weight.arrived(6)
        weight.start(8)

    def near_multiply(at):
        weights[at].arrived(3)
        multiply(at, 1)
        weights[at].arrived(4)
        multiply(at, 2)

    def far_multiply(at):
        weights[at].arrived(7, 8)
        multiply(at, 3)

    loads[2].wait()
    loads[3].wait()
    fetch.wait()
    query.arrived(2)
    multiply(0, 0)
    key.arrived(2)
    multiply(1, 0)
    near(query)
    near_multiply(0)
    near(key)
    value.start(2, 0, 1)
    output.start(2, 0, 1)
    near_multiply(1)
    value.arrived(2)
    multiply(2, 0)
    far(query)
    far_multiply(0)
    far(key)
    far_multiply(1)
    near(value)
    near_multiply(2)
    near(output)
    far(value)
    far_multiply(2)
    value_ref[...] = value_sum[...].astype(value_ref.dtype)
    output.arrived(2, 3, 4)
    far(output)
    output.arrived(7, 8)
    for weight in weights:
        weight.sent()


def project(tokens, query_weight, key_weight, value_weight, output_weight, stride):
    count = tokens.shape[0]
    rows, width = query_weight.shape
    output_rows, output_width = output_weight.shape
    anywhere = pl.BlockSpec(memory_space=pl.ANY)
    vmem = pl.BlockSpec(memory_space=pltpu.VMEM)
    query, key, value, output = pl.pallas_call(
        functools.partial(project_kernel, stride),
        out_shape=(
            jax.ShapeDtypeStruct((count, width), jnp.float32),
            jax.ShapeDtypeStruct((count, width), jnp.float32),
            jax.ShapeDtypeStruct((count, width), jnp.bfloat16),
            jax.ShapeDtypeStruct((CUBE // 2, 2 * output_rows, output_width), jnp.bfloat16),
        ),
        in_specs=[anywhere] * 5,
        out_specs=(vmem, vmem, vmem, anywhere),
        scratch_shapes=[
            pltpu.VMEM(tokens.shape, tokens.dtype),
            pltpu.VMEM((3, CUBE // 2, 2 * rows, width), query_weight.dtype),
            pltpu.VMEM((count, width), jnp.float32),
            pltpu.SemaphoreType.DMA((5,)),
            pltpu.SemaphoreType.DMA((4, 9)),
            pltpu.SemaphoreType.DMA((4, 9)),
        ],
        compiler_params=pltpu.CompilerParams(
            collective_id=0, has_side_effects=True, vmem_limit_bytes=60 * 1024 * 1024
        ),
        name="project",
    )(tokens, query_weight, key_weight, value_weight, output_weight)
    return query, key, value, output.reshape(-1, output_width)


def pregather(weight, stride):
    if stride == 1:
        return weight
    count = lax.axis_size("hw")
    groups = [list(range(first, first + stride)) for first in range(0, count, stride)]
    return lax.all_gather(weight, "hw", axis=0, tiled=True, axis_index_groups=groups)


def per_device(
    latents,
    query_weight,
    key_weight,
    value_weight,
    output_weight,
    query_gain,
    key_gain,
    frame_index,
    row_index,
    column_index,
):
    frames, side, width = (latents.shape[1], latents.shape[2], latents.shape[4])
    tokens = latents.reshape(frames * side * side, width)
    head_dim = HD
    full_width = HEADS * HD
    group_width = query_weight.shape[1]
    heads_here = group_width // head_dim
    grid_columns = lax.axis_size("hw") // DEV_ROWS
    place = lax.axis_index("hw")
    grid_row = place // grid_columns
    grid_column = place % grid_columns
    tiles_side = side // WT
    stride = lax.axis_size("hw") // CUBE
    query_lin, key_lin, values, output_all = project(
        tokens,
        *(pregather(w, stride) for w in (query_weight, key_weight, value_weight, output_weight)),
        stride,
    )
    query_squares, key_squares = lax.psum(
        (jnp.sum(query_lin * query_lin, axis=1), jnp.sum(key_lin * key_lin, axis=1)), "head"
    )
    query_norm = query_lin * lax.rsqrt(query_squares / full_width + NORM_EPS)[:, None] * query_gain
    key_norm = key_lin * lax.rsqrt(key_squares / full_width + NORM_EPS)[:, None] * key_gain
    rows_here = lax.dynamic_slice_in_dim(row_index, grid_row * side, side)
    columns_here = lax.dynamic_slice_in_dim(column_index, grid_column * side, side)
    angle = rope_angles(frame_index, rows_here, columns_here, head_dim)
    queries_grid = rotate(query_norm, angle, heads_here, head_dim)
    keys_grid = rotate(key_norm, angle, heads_here, head_dim)
    values_grid = values.reshape(frames, side, side, group_width)
    stack = jnp.stack([keys_grid, values_grid])
    received = {}
    for down in (-1, 0, 1):
        for right in (-1, 0, 1):
            if down != 0 or right != 0:
                received[down, right] = from_behind(
                    region(stack, down, right, WT), "hw", -(down * grid_columns + right)
                )
    received[0, 0] = stack
    bands = [
        jnp.concatenate([received[down, right] for right in (-1, 0, 1)], axis=3)
        for down in (-1, 0, 1)
    ]
    padded = jnp.concatenate(bands, axis=2)
    spatial = window_attend(
        queries_grid,
        padded[0],
        padded[1],
        grid_row * tiles_side,
        grid_column * tiles_side,
        DEV_ROWS * tiles_side,
        grid_columns * tiles_side,
        heads_here,
        head_dim,
    )
    mixed = frame_attend(queries_grid, keys_grid, spatial, heads_here, head_dim)
    gathered = lax.all_gather(mixed.reshape(-1, group_width), "head", axis=1, tiled=True)
    result = jnp.dot(gathered, output_all, preferred_element_type=jnp.float32)
    return result.astype(jnp.bfloat16).reshape(1, frames, side, side, output_weight.shape[1])


def solution(mesh):
    placed = (
        P("hw", None, None, None, None),
        P("hw", "head"),
        P("hw", "head"),
        P("hw", "head"),
        P("hw", "head"),
        P("head"),
        P("head"),
        P(),
        P(),
        P(),
    )
    return jax.shard_map(
        per_device,
        mesh=mesh,
        in_specs=placed,
        out_specs=P("hw", None, None, None, "head"),
        check_vma=False,
    )
```

```python
import functools
import math

import jax
import jax.numpy as jnp
from jax import lax
from jax.experimental import pallas as pl
from jax.experimental.pallas import tpu as pltpu
from jax.sharding import PartitionSpec as P

HEADS = 20
HD = 128
WT = 4
DEV_ROWS = 4


NORM_EPS = 0.5


def from_behind(value, axis, steps):
    count = lax.axis_size(axis)
    initial, last = (max(0, -steps), min(count, count - steps))
    return lax.ppermute(value, axis, [(source, source + steps) for source in range(initial, last)])


def freq_table(count):
    ratios = jnp.arange(count, dtype=jnp.float32) / count
    return jnp.float32(10000.0) ** (-ratios)


def rope_angles(frame_index, row_index, column_index, head_dim):
    side_pairs = head_dim // 6
    frame_pairs = head_dim // 2 - 2 * side_pairs
    frame_part = frame_index.astype(jnp.float32)[:, None] * freq_table(frame_pairs)[None, :]
    row_part = row_index.astype(jnp.float32)[:, None] * freq_table(side_pairs)[None, :]
    column_part = column_index.astype(jnp.float32)[:, None] * freq_table(side_pairs)[None, :]
    frames, rows, columns = (frame_part.shape[0], row_part.shape[0], column_part.shape[0])
    return jnp.concatenate(
        [
            jnp.broadcast_to(frame_part[:, None, None, :], (frames, rows, columns, frame_pairs)),
            jnp.broadcast_to(row_part[None, :, None, :], (frames, rows, columns, side_pairs)),
            jnp.broadcast_to(column_part[None, None, :, :], (frames, rows, columns, side_pairs)),
        ],
        axis=-1,
    )


def pair_turn(head_dim):
    source = jnp.arange(head_dim)[:, None]
    target = jnp.arange(head_dim)[None, :]
    plus = ((target % 2 == 1) & (source == target - 1)).astype(jnp.float32)
    minus = ((target % 2 == 0) & (source == target + 1)).astype(jnp.float32)
    return plus - minus


def rotate(features, angle, heads_here, head_dim):
    frames, rows, columns = (angle.shape[0], angle.shape[1], angle.shape[2])
    cosine = jnp.repeat(jnp.cos(angle), 2, axis=-1)[:, :, :, None, :]
    sine = jnp.repeat(jnp.sin(angle), 2, axis=-1)[:, :, :, None, :]
    shaped = features.reshape(frames, rows, columns, heads_here, head_dim)
    turned = jnp.dot(
        shaped.reshape(-1, head_dim), pair_turn(head_dim), precision=lax.Precision.HIGHEST
    ).reshape(shaped.shape)
    rotated = shaped * cosine + turned * sine
    return rotated.astype(jnp.bfloat16).reshape(frames, rows, columns, heads_here * head_dim)


def region(stack, down, right, edge):
    rows = stack.shape[2]
    columns = stack.shape[3]
    row_start, row_stop = (rows - edge, rows) if down < 0 else (0, edge) if down > 0 else (0, rows)
    column_start, column_stop = (
        (columns - edge, columns) if right < 0 else (0, edge) if right > 0 else (0, columns)
    )
    return stack[:, :, row_start:row_stop, column_start:column_stop]


CUBE = 8


class Cube:
    def __init__(self, stride):
        me = lax.axis_index("hw")
        within = lax.rem(me, stride) if stride > 1 else 0
        place = lax.div(me, stride) if stride > 1 else me
        core = lax.rem(place, 2)
        x = lax.rem(lax.div(place, 2), 2)
        y = lax.div(place, 4)
        self.place = place
        self.other = [place + 1 - 2 * core, place + 2 - 4 * x, place + 4 - 8 * y]
        self.diagonal = place + 2 - 4 * x + 4 - 8 * y
        self.devices = [{"hw": other * stride + within} for other in self.other]
        self.chip = lax.div(place, 2)
        self.chips = [
            self.chip,
            self.chip + 1 - 2 * x,
            self.chip + 2 - 4 * y,
            self.chip + 3 - 2 * x - 4 * y,
        ]

    def barrier(self, line=None):
        semaphore = pltpu.get_barrier_semaphore()
        if line is not None:
            line.greet(semaphore)
        for device in self.devices:
            pl.semaphore_signal(semaphore, inc=1, device_id=device, device_id_type=pl.DeviceIdType.MESH)
        if line is None:
            pl.semaphore_wait(semaphore, len(self.devices))
        else:
            line.meet(semaphore, len(self.devices))


class Exchange:
    def __init__(self, cube, held, send, receive, rows):
        core_place, x_place, y_place = cube.other
        half = rows // 2

        def part(place, low, size):
            start = pl.multiple_of(lax.rem(place, 2) * rows + low, 16)
            return held.at[lax.div(place, 2), pl.ds(start, size)]

        def copy(at, place, low, size, partner):
            ref = part(place, low, size)
            return pltpu.make_async_remote_copy(
                src_ref=ref,
                dst_ref=ref,
                send_sem=send.at[at],
                recv_sem=receive.at[at],
                device_id=cube.devices[partner],
                device_id_type=pl.DeviceIdType.MESH,
            )

        self.own = part(cube.place, 0, rows)
        self.copies = [
            copy(0, cube.place, 0, rows, 1),
            copy(1, cube.place, 0, rows, 2),
            copy(2, cube.place, 0, rows, 0),
            copy(3, x_place, 0, rows, 0),
            copy(4, y_place, 0, rows, 0),
            copy(5, x_place, 0, half, 2),
            copy(6, y_place, half, half, 1),
            copy(7, cube.diagonal, 0, half, 0),
            copy(8, cube.diagonal, half, half, 0),
        ]

    def start(self, *which):
        for at in which:
            self.copies[at].start()

    def arrived(self, *which):
        for at in which:
            self.copies[at].wait_recv()

    def near(self):
        self.arrived(0)
        self.start(5, 3)
        self.arrived(1)
        self.start(6, 4)

    def far(self):
        self.arrived(5)
        self.start(7)
        self.arrived(6)
        self.start(8)

    def sent(self):
        for one in self.copies:
            one.wait_send()


def project_kernel(
    stride, tokens_hbm, query_hbm, key_hbm, value_hbm,
    query_ref, key_ref, value_ref,
    tokens, held, value_sum, local, send, receive,
):
    cube = Cube(stride)
    rows = query_hbm.shape[0]
    depth = 2 * rows
    weights = [
        Exchange(cube, held.at[at], send.at[at], receive.at[at], rows) for at in range(3)
    ]
    loads = [
        pltpu.make_async_copy(source, weight.own, local.at[at])
        for at, (source, weight) in enumerate(
            zip((query_hbm, key_hbm, value_hbm), weights)
        )
    ]
    fetch = pltpu.make_async_copy(tokens_hbm, tokens, local.at[3])
    for load in loads:
        load.start()
    fetch.start()
    cube.barrier()
    query, key, value = weights
    loads[0].wait()
    query.start(2, 0, 1)
    loads[1].wait()
    key.start(2, 0, 1)
    sums = [query_ref, key_ref, value_sum]
    block = tokens.shape[0] // 2

    def multiply(at, lane):
        chip = cube.chips[lane]

        @pl.loop(0, 2)
        def _(step):
            here = pl.ds(pl.multiple_of(step * block, block), block)
            product = jnp.dot(
                tokens[here, pl.ds(pl.multiple_of(chip * depth, 128), depth)],
                held[at, chip],
                preferred_element_type=jnp.float32,
            )
            if lane == 0:
                sums[at][here, :] = product
            else:
                sums[at][here, :] += product

    def near_multiply(at):
        weights[at].arrived(3)
        multiply(at, 1)
        weights[at].arrived(4)
        multiply(at, 2)

    def far_multiply(at):
        weights[at].arrived(7, 8)
        multiply(at, 3)

    loads[2].wait()
    fetch.wait()
    query.arrived(2)
    multiply(0, 0)
    key.arrived(2)
    multiply(1, 0)
    query.near()
    near_multiply(0)
    key.near()
    value.start(2, 0, 1)
    near_multiply(1)
    value.arrived(2)
    multiply(2, 0)
    query.far()
    far_multiply(0)
    key.far()
    far_multiply(1)
    value.near()
    near_multiply(2)
    value.far()
    far_multiply(2)
    value_ref[...] = value_sum[...].astype(value_ref.dtype)
    for weight in weights:
        weight.sent()


def project(tokens, query_weight, key_weight, value_weight, stride):
    count = tokens.shape[0]
    rows, width = query_weight.shape
    anywhere = pl.BlockSpec(memory_space=pl.ANY)
    vmem = pl.BlockSpec(memory_space=pltpu.VMEM)
    return pl.pallas_call(
        functools.partial(project_kernel, stride),
        out_shape=(
            jax.ShapeDtypeStruct((count, width), jnp.float32),
            jax.ShapeDtypeStruct((count, width), jnp.float32),
            jax.ShapeDtypeStruct((count, width), jnp.bfloat16),
        ),
        in_specs=[anywhere] * 4,
        out_specs=(vmem, vmem, vmem),
        scratch_shapes=[
            pltpu.VMEM(tokens.shape, tokens.dtype),
            pltpu.VMEM((3, CUBE // 2, 2 * rows, width), query_weight.dtype),
            pltpu.VMEM((count, width), jnp.float32),
            pltpu.SemaphoreType.DMA((4,)),
            pltpu.SemaphoreType.DMA((3, 9)),
            pltpu.SemaphoreType.DMA((3, 9)),
        ],
        compiler_params=pltpu.CompilerParams(
            collective_id=0, has_side_effects=True, vmem_limit_bytes=60 * 1024 * 1024
        ),
        name="project",
    )(tokens, query_weight, key_weight, value_weight)


class Line:
    def __init__(self, blocks, send, receive):
        self.count = lax.axis_size("head")
        self.me = lax.axis_index("head")
        self.blocks, self.send, self.receive = blocks, send, receive

    def neighbour(self, side):
        return self.me + 1 if side == 0 else self.me - 1

    def has(self, side):
        return self.me < self.count - 1 if side == 0 else self.me > 0

    def greet(self, semaphore):
        for side in range(2):
            @pl.when(self.has(side))
            def _():
                pl.semaphore_signal(
                    semaphore,
                    inc=1,
                    device_id={"head": self.neighbour(side)},
                    device_id_type=pl.DeviceIdType.MESH,
                )

    def meet(self, semaphore, others):
        both = self.has(0) & self.has(1)

        @pl.when(both)
        def _():
            pl.semaphore_wait(semaphore, others + 2)

        @pl.when(jnp.logical_not(both))
        def _():
            pl.semaphore_wait(semaphore, others + 1)

    def origin(self, side, far):
        return self.me - far if side == 0 else self.me + far

    def holds(self, side, far):
        return self.me >= far if side == 0 else self.me + far < self.count

    def copy(self, side, far, at, group):
        ref = self.blocks(group, at)
        return pltpu.make_async_remote_copy(
            src_ref=ref,
            dst_ref=ref,
            send_sem=self.send.at[side, far, at],
            recv_sem=self.receive.at[side, far, at],
            device_id={"head": self.neighbour(side)},
            device_id_type=pl.DeviceIdType.MESH,
        )

    def start(self, side, far, at):
        @pl.when(self.has(side) & self.holds(side, far))
        def _():
            self.copy(side, far, at, self.origin(side, far)).start()

    def relay(self, far, at):
        for side in range(2):
            @pl.when(self.holds(side, far + 1))
            def _():
                self.copy(side, far, at, self.origin(side, far + 1)).wait_recv()

            if far + 2 < self.count:
                self.start(side, far + 1, at)

    def sent(self, parts):
        for side in range(2):
            for far in range(self.count - 1):
                @pl.when(self.has(side) & self.holds(side, far))
                def _():
                    @pl.loop(0, parts)
                    def _(at):
                        self.copy(side, far, at, self.origin(side, far)).wait_send()


def weigh(scores, allowed):
    scores = jnp.where(allowed, scores, -jnp.inf)
    raised = jnp.exp(scores - jnp.max(scores, axis=-1, keepdims=True))
    return (raised * (1.0 / jnp.sum(raised, axis=-1, keepdims=True))).astype(jnp.bfloat16)


def score(queries, keys):
    return lax.dot_general(
        queries, keys, (((1,), (1,)), ((), ())), preferred_element_type=jnp.float32
    ) * (1.0 / math.sqrt(HD))


def attend_kernel(
    stride, grid_columns, frames, side,
    query_ref, key_ref, key_pad, value_pad, output_hbm,
    result_ref,
    spatial, mixed, held, total, local, send, receive, line_send, line_receive,
):
    cube = Cube(stride)
    rows, columns = output_hbm.shape
    weight = Exchange(cube, held, send, receive, rows)
    load = pltpu.make_async_copy(output_hbm, weight.own, local)
    load.start()
    group_width = query_ref.shape[1]
    heads_here = group_width // HD
    tokens = query_ref.shape[0]

    def head_of(at):
        return pl.ds(pl.multiple_of(at * HD, HD), HD)

    line = Line(lambda group, at: mixed.at[group, :, head_of(at)], line_send, line_receive)
    cube.barrier(line)
    load.wait()
    weight.start(2, 0, 1)

    area = side * side
    wide = side + 2 * WT
    window = wide * wide
    place = lax.axis_index("hw")
    tile_row = lax.div(place, grid_columns) * (side // WT) - 1
    tile_column = lax.rem(place, grid_columns) * (side // WT) - 1
    query_at = lax.broadcasted_iota(jnp.int32, (area, window), 0)
    key_at = lax.broadcasted_iota(jnp.int32, (area, window), 1)
    key_row, key_column = key_at // wide // WT, key_at % wide // WT
    down = key_row - query_at // side // WT
    right = key_column - query_at % side // WT
    near = (down >= 0) & (down <= 2) & (right >= 0) & (right <= 2)
    near &= (key_row + tile_row >= 0) & (key_row + tile_row < DEV_ROWS * (side // WT))
    near &= (key_column + tile_column >= 0) & (
        key_column + tile_column < grid_columns * (side // WT)
    )
    strip = 2 * area
    same = (
        lax.broadcasted_iota(jnp.int32, (strip, tokens), 0) % area
        == lax.broadcasted_iota(jnp.int32, (strip, tokens), 1) % area
    )

    @pl.loop(0, heads_here)
    def _(at):
        head = head_of(at)
        scores = [
            score(query_ref[pl.ds(frame * area, area), head], key_pad[frame, :, head])
            for frame in range(frames)
        ]
        weights = [weigh(one, near) for one in scores]
        for frame in range(frames):
            spatial[pl.ds(frame * area, area), :] = jnp.dot(
                weights[frame], value_pad[frame, :, head], preferred_element_type=jnp.float32
            ).astype(jnp.bfloat16)
        for low in range(0, tokens, strip):
            over = weigh(score(query_ref[pl.ds(low, strip), head], key_ref[:, head]), same)
            mixed[line.me, pl.ds(low, strip), head] = jnp.dot(
                over, spatial[...], preferred_element_type=jnp.float32
            ).astype(jnp.bfloat16)
        line.start(0, 0, at)
        line.start(1, 0, at)

    block = tokens // 2

    def multiply(group, first=False):
        @pl.loop(0, 2)
        def _(step):
            here = pl.ds(pl.multiple_of(step * block, block), block)
            product = jnp.dot(mixed[group, here, :], held[group], preferred_element_type=jnp.float32)
            if first:
                total[here, :] = product
            else:
                total[here, :] += product

    def relay(far):
        @pl.loop(0, heads_here)
        def _(at):
            line.relay(far, at)

    relay(0)
    weight.near()
    weight.arrived(2, 3, 4)
    if line.count > 2:
        relay(1)
    weight.far()
    weight.arrived(7, 8)
    multiply(line.me, True)
    for far in range(line.count - 1):
        if far > 1:
            relay(far)
        for side_at in range(2):
            @pl.when(line.holds(side_at, far + 1))
            def _():
                multiply(line.origin(side_at, far + 1))
    result_ref[...] = total[...].astype(result_ref.dtype)
    weight.sent()
    line.sent(heads_here)


def attend(queries, keys, key_pad, value_pad, output_weight, stride, grid_columns, frames, side):
    tokens, group_width = queries.shape
    rows, columns = output_weight.shape
    groups = lax.axis_size("head")
    heads_here = group_width // HD
    vmem = pl.BlockSpec(memory_space=pltpu.VMEM)
    return pl.pallas_call(
        functools.partial(attend_kernel, stride, grid_columns, frames, side),
        out_shape=jax.ShapeDtypeStruct((tokens, columns), jnp.bfloat16),
        in_specs=[vmem] * 4 + [pl.BlockSpec(memory_space=pl.ANY)],
        out_specs=vmem,
        scratch_shapes=[
            pltpu.VMEM((tokens, HD), jnp.bfloat16),
            pltpu.VMEM((groups, tokens, group_width), jnp.bfloat16),
            pltpu.VMEM((CUBE // 2, 2 * rows, columns), output_weight.dtype),
            pltpu.VMEM((tokens, columns), jnp.float32),
            pltpu.SemaphoreType.DMA,
            pltpu.SemaphoreType.DMA((9,)),
            pltpu.SemaphoreType.DMA((9,)),
            pltpu.SemaphoreType.DMA((2, groups - 1, heads_here)),
            pltpu.SemaphoreType.DMA((2, groups - 1, heads_here)),
        ],
        compiler_params=pltpu.CompilerParams(
            collective_id=1, has_side_effects=True, vmem_limit_bytes=60 * 1024 * 1024
        ),
        name="attend",
    )(queries, keys, key_pad, value_pad, output_weight)


def pregather(weight, stride):
    if stride == 1:
        return weight
    count = lax.axis_size("hw")
    groups = [list(range(first, first + stride)) for first in range(0, count, stride)]
    return lax.all_gather(weight, "hw", axis=0, tiled=True, axis_index_groups=groups)


def per_device(
    latents,
    query_weight,
    key_weight,
    value_weight,
    output_weight,
    query_gain,
    key_gain,
    frame_index,
    row_index,
    column_index,
):
    frames, side, width = (latents.shape[1], latents.shape[2], latents.shape[4])
    tokens = latents.reshape(frames * side * side, width)
    head_dim = HD
    full_width = HEADS * HD
    group_width = query_weight.shape[1]
    heads_here = group_width // head_dim
    grid_columns = lax.axis_size("hw") // DEV_ROWS
    place = lax.axis_index("hw")
    grid_row = place // grid_columns
    grid_column = place % grid_columns
    stride = lax.axis_size("hw") // CUBE
    query_lin, key_lin, values = project(
        tokens,
        *(pregather(w, stride) for w in (query_weight, key_weight, value_weight)),
        stride,
    )
    query_squares, key_squares = lax.psum(
        (jnp.sum(query_lin * query_lin, axis=1), jnp.sum(key_lin * key_lin, axis=1)), "head"
    )
    query_norm = query_lin * lax.rsqrt(query_squares / full_width + NORM_EPS)[:, None] * query_gain
    key_norm = key_lin * lax.rsqrt(key_squares / full_width + NORM_EPS)[:, None] * key_gain
    rows_here = lax.dynamic_slice_in_dim(row_index, grid_row * side, side)
    columns_here = lax.dynamic_slice_in_dim(column_index, grid_column * side, side)
    angle = rope_angles(frame_index, rows_here, columns_here, head_dim)
    queries_grid = rotate(query_norm, angle, heads_here, head_dim)
    keys_grid = rotate(key_norm, angle, heads_here, head_dim)
    values_grid = values.reshape(frames, side, side, group_width)
    stack = jnp.stack([keys_grid, values_grid])
    received = {}
    for down in (-1, 0, 1):
        for right in (-1, 0, 1):
            if down != 0 or right != 0:
                received[down, right] = from_behind(
                    region(stack, down, right, WT), "hw", -(down * grid_columns + right)
                )
    received[0, 0] = stack
    bands = [
        jnp.concatenate([received[down, right] for right in (-1, 0, 1)], axis=3)
        for down in (-1, 0, 1)
    ]
    padded = jnp.concatenate(bands, axis=2)
    result = attend(
        queries_grid.reshape(-1, group_width),
        keys_grid.reshape(-1, group_width),
        padded[0].reshape(frames, -1, group_width),
        padded[1].reshape(frames, -1, group_width),
        pregather(output_weight, stride),
        stride,
        grid_columns,
        frames,
        side,
    )
    return result.reshape(1, frames, side, side, output_weight.shape[1])


def solution(mesh):
    placed = (
        P("hw", None, None, None, None),
        P("hw", "head"),
        P("hw", "head"),
        P("hw", "head"),
        P("hw", "head"),
        P("head"),
        P("head"),
        P(),
        P(),
        P(),
    )
    return jax.shard_map(
        per_device,
        mesh=mesh,
        in_specs=placed,
        out_specs=P("hw", None, None, None, "head"),
        check_vma=False,
    )
```

```python
import functools
import math

import jax
import jax.numpy as jnp
from jax import lax
from jax.experimental import pallas as pl
from jax.experimental.pallas import tpu as pltpu
from jax.sharding import PartitionSpec as P

HEADS = 20
HD = 128
WT = 4
DEV_ROWS = 4


NORM_EPS = 0.5


def freq_table(count):
    ratios = jnp.arange(count, dtype=jnp.float32) / count
    return jnp.float32(10000.0) ** (-ratios)


def rope_angles(frame_index, row_index, column_index, head_dim):
    side_pairs = head_dim // 6
    frame_pairs = head_dim // 2 - 2 * side_pairs

    def lanes(before, count, after):
        return jnp.repeat(jnp.pad(freq_table(count), (before, after)), 2)

    frame_part = frame_index.astype(jnp.float32)[:, None] * lanes(0, frame_pairs, 2 * side_pairs)
    row_part = row_index.astype(jnp.float32)[:, None] * lanes(frame_pairs, side_pairs, side_pairs)
    column_part = column_index.astype(jnp.float32)[:, None] * lanes(
        frame_pairs + side_pairs, side_pairs, 0
    )
    total = frame_part[:, None, None] + row_part[:, None] + column_part
    return total.reshape(-1, head_dim)


def rotate(features, cosine, sine, heads_here, head_dim):
    even = lax.broadcasted_iota(jnp.int32, cosine.shape, 1) % 2 == 0
    heads = []
    for head in range(heads_here):
        one = features[:, head * head_dim : (head + 1) * head_dim]
        turned = jnp.where(even, -jnp.roll(one, -1, axis=1), jnp.roll(one, 1, axis=1))
        heads.append((one * cosine + turned * sine).astype(jnp.bfloat16))
    return jnp.concatenate(heads, axis=1)


CUBE = 8


class Cube:
    def __init__(self, stride):
        me = lax.axis_index("hw")
        within = lax.rem(me, stride) if stride > 1 else 0
        place = lax.div(me, stride) if stride > 1 else me
        core = lax.rem(place, 2)
        x = lax.rem(lax.div(place, 2), 2)
        y = lax.div(place, 4)
        self.place = place
        self.other = [place + 1 - 2 * core, place + 2 - 4 * x, place + 4 - 8 * y]
        self.diagonal = place + 2 - 4 * x + 4 - 8 * y
        self.devices = [{"hw": other * stride + within} for other in self.other]
        self.chip = lax.div(place, 2)
        self.chips = [
            self.chip,
            self.chip + 1 - 2 * x,
            self.chip + 2 - 4 * y,
            self.chip + 3 - 2 * x - 4 * y,
        ]

    def barrier(self, line=None):
        semaphore = pltpu.get_barrier_semaphore()
        if line is not None:
            for peers in line:
                peers.greet(semaphore)
        for device in self.devices:
            pl.semaphore_signal(semaphore, inc=1, device_id=device, device_id_type=pl.DeviceIdType.MESH)
        if line is None:
            pl.semaphore_wait(semaphore, len(self.devices))
        else:
            count = sum((peers.number() for peers in line), len(self.devices))
            pl.semaphore_wait(semaphore, count)


class Exchange:
    def __init__(self, cube, held, send, receive, rows):
        core_place, x_place, y_place = cube.other
        half = rows // 2

        def part(place, low, size):
            start = pl.multiple_of(lax.rem(place, 2) * rows + low, 16)
            return held.at[lax.div(place, 2), pl.ds(start, size)]

        def copy(at, place, low, size, partner):
            ref = part(place, low, size)
            return pltpu.make_async_remote_copy(
                src_ref=ref,
                dst_ref=ref,
                send_sem=send.at[at],
                recv_sem=receive.at[at],
                device_id=cube.devices[partner],
                device_id_type=pl.DeviceIdType.MESH,
            )

        self.own = part(cube.place, 0, rows)
        self.copies = [
            copy(0, cube.place, 0, rows, 1),
            copy(1, cube.place, 0, rows, 2),
            copy(2, cube.place, 0, rows, 0),
            copy(3, x_place, 0, rows, 0),
            copy(4, y_place, 0, rows, 0),
            copy(5, x_place, 0, half, 2),
            copy(6, y_place, half, half, 1),
            copy(7, cube.diagonal, 0, half, 0),
            copy(8, cube.diagonal, half, half, 0),
        ]

    def start(self, *which):
        for at in which:
            self.copies[at].start()

    def arrived(self, *which):
        for at in which:
            self.copies[at].wait_recv()

    def near(self):
        self.arrived(0)
        self.start(5, 3)
        self.arrived(1)
        self.start(6, 4)

    def far(self):
        self.arrived(5)
        self.start(7)
        self.arrived(6)
        self.start(8)

    def sent(self):
        for one in self.copies:
            one.wait_send()


def project_kernel(
    stride, tokens_hbm, query_hbm, key_hbm, value_hbm,
    query_ref, key_ref, value_ref,
    tokens, held, value_sum, local, send, receive,
):
    cube = Cube(stride)
    rows = query_hbm.shape[0]
    depth = 2 * rows
    weights = [
        Exchange(cube, held.at[at], send.at[at], receive.at[at], rows) for at in range(3)
    ]
    loads = [
        pltpu.make_async_copy(source, weight.own, local.at[at])
        for at, (source, weight) in enumerate(
            zip((query_hbm, key_hbm, value_hbm), weights)
        )
    ]
    fetch = pltpu.make_async_copy(tokens_hbm, tokens, local.at[3])
    for load in loads:
        load.start()
    fetch.start()
    cube.barrier()
    query, key, value = weights
    loads[0].wait()
    query.start(2, 0, 1)
    loads[1].wait()
    key.start(2, 0, 1)
    sums = [query_ref, key_ref, value_sum]
    block = tokens.shape[0] // 2

    def multiply(at, lane):
        chip = cube.chips[lane]

        @pl.loop(0, 2)
        def _(step):
            here = pl.ds(pl.multiple_of(step * block, block), block)
            product = jnp.dot(
                tokens[here, pl.ds(pl.multiple_of(chip * depth, 128), depth)],
                held[at, chip],
                preferred_element_type=jnp.float32,
            )
            if lane == 0:
                sums[at][here, :] = product
            else:
                sums[at][here, :] += product

    def near_multiply(at):
        weights[at].arrived(3)
        multiply(at, 1)
        weights[at].arrived(4)
        multiply(at, 2)

    def far_multiply(at):
        weights[at].arrived(7, 8)
        multiply(at, 3)

    loads[2].wait()
    fetch.wait()
    query.arrived(2)
    multiply(0, 0)
    key.arrived(2)
    multiply(1, 0)
    query.near()
    near_multiply(0)
    key.near()
    value.start(2, 0, 1)
    near_multiply(1)
    value.arrived(2)
    multiply(2, 0)
    query.far()
    far_multiply(0)
    key.far()
    far_multiply(1)
    value.near()
    near_multiply(2)
    value.far()
    far_multiply(2)
    value_ref[...] = value_sum[...].astype(value_ref.dtype)
    for weight in weights:
        weight.sent()


def project(tokens, query_weight, key_weight, value_weight, stride):
    count = tokens.shape[0]
    rows, width = query_weight.shape
    anywhere = pl.BlockSpec(memory_space=pl.ANY)
    vmem = pl.BlockSpec(memory_space=pltpu.VMEM)
    return pl.pallas_call(
        functools.partial(project_kernel, stride),
        out_shape=(
            jax.ShapeDtypeStruct((count, width), jnp.float32),
            jax.ShapeDtypeStruct((count, width), jnp.float32),
            jax.ShapeDtypeStruct((count, width), jnp.bfloat16),
        ),
        in_specs=[anywhere] * 4,
        out_specs=(vmem, vmem, vmem),
        scratch_shapes=[
            pltpu.VMEM(tokens.shape, tokens.dtype),
            pltpu.VMEM((3, CUBE // 2, 2 * rows, width), query_weight.dtype),
            pltpu.VMEM((count, width), jnp.float32),
            pltpu.SemaphoreType.DMA((4,)),
            pltpu.SemaphoreType.DMA((3, 9)),
            pltpu.SemaphoreType.DMA((3, 9)),
        ],
        compiler_params=pltpu.CompilerParams(
            collective_id=0, has_side_effects=True, vmem_limit_bytes=60 * 1024 * 1024
        ),
        name="project",
    )(tokens, query_weight, key_weight, value_weight)


class Line:
    def __init__(self, blocks, send, receive):
        self.count = lax.axis_size("head")
        self.me = lax.axis_index("head")
        self.blocks, self.send, self.receive = blocks, send, receive

    def neighbour(self, side):
        return self.me + 1 if side == 0 else self.me - 1

    def has(self, side):
        return self.me < self.count - 1 if side == 0 else self.me > 0

    def greet(self, semaphore):
        for side in range(2):
            @pl.when(self.has(side))
            def _():
                pl.semaphore_signal(
                    semaphore,
                    inc=1,
                    device_id={"head": self.neighbour(side)},
                    device_id_type=pl.DeviceIdType.MESH,
                )

    def number(self):
        return ones(self.me, self.count)

    def origin(self, side, far):
        return self.me - far if side == 0 else self.me + far

    def holds(self, side, far):
        return self.me >= far if side == 0 else self.me + far < self.count

    def copy(self, side, far, at, group):
        ref = self.blocks(group, at)
        return pltpu.make_async_remote_copy(
            src_ref=ref,
            dst_ref=ref,
            send_sem=self.send.at[side, far, at],
            recv_sem=self.receive.at[side, far, at],
            device_id={"head": self.neighbour(side)},
            device_id_type=pl.DeviceIdType.MESH,
        )

    def start(self, side, far, at):
        @pl.when(self.has(side) & self.holds(side, far))
        def _():
            self.copy(side, far, at, self.origin(side, far)).start()

    def relay(self, far, at):
        for side in range(2):
            @pl.when(self.holds(side, far + 1))
            def _():
                self.copy(side, far, at, self.origin(side, far + 1)).wait_recv()

            if far + 2 < self.count:
                self.start(side, far + 1, at)

    def sent(self, parts):
        for side in range(2):
            for far in range(self.count - 1):
                @pl.when(self.has(side) & self.holds(side, far))
                def _():
                    @pl.loop(0, parts)
                    def _(at):
                        self.copy(side, far, at, self.origin(side, far)).wait_send()


def ones(me, count):
    return 1 - lax.div(me + 1, count) + lax.div(me + count - 1, count)


class Halo:
    def __init__(self, sources, pads, grid_columns, side, local, send, receive, side_send, side_receive):
        place = lax.axis_index("hw")
        self.row, self.column = lax.div(place, grid_columns), lax.rem(place, grid_columns)
        self.place, self.columns = place, grid_columns
        self.sources, self.pads = sources, pads
        self.edge, self.body = WT * side, side * side
        self.slots = min(3, grid_columns)
        self.own = self.column if grid_columns == 2 else self.slots // 2
        self.local, self.send, self.receive = local, send, receive
        self.side_send, self.side_receive = side_send, side_receive
        self.parts = [
            pl.ds(self.edge, self.body),
            pl.ds(0, self.edge),
            pl.ds(self.edge + self.body, self.edge),
        ]

    def first_column(self):
        return 0 if self.columns == 2 else self.column - self.slots // 2

    def has(self, way):
        return [
            self.row > 0,
            self.row < DEV_ROWS - 1,
            self.column > 0,
            self.column < self.columns - 1,
        ][way]

    def device(self, way):
        step = [-self.columns, self.columns, -1, 1][way]
        return {"hw": self.place + step}

    def greet(self, semaphore):
        for way in range(4):
            @pl.when(self.has(way))
            def _():
                pl.semaphore_signal(
                    semaphore,
                    inc=1,
                    device_id=self.device(way),
                    device_id_type=pl.DeviceIdType.MESH,
                )

    def number(self):
        return ones(self.row, DEV_ROWS) + ones(self.column, self.columns)

    def vertical(self, kind, way):
        low = 0 if way == 0 else self.body - self.edge
        return pltpu.make_async_remote_copy(
            src_ref=self.sources[kind].at[:, pl.ds(low, self.edge), :],
            dst_ref=self.pads[kind].at[self.own, :, self.parts[2 - way], :],
            send_sem=self.send.at[kind, way],
            recv_sem=self.receive.at[kind, way],
            device_id=self.device(way),
            device_id_type=pl.DeviceIdType.MESH,
        )

    def sideways(self, kind, way, part):
        own = self.pads[kind].at[self.own, :, self.parts[part], :]
        if self.columns == 2:
            slot = self.own
        else:
            slot = self.slots - 1 if way == 2 else 0
        return pltpu.make_async_remote_copy(
            src_ref=self.sources[kind] if part == 0 else own,
            dst_ref=self.pads[kind].at[slot, :, self.parts[part], :],
            send_sem=self.side_send.at[kind, way - 2, part],
            recv_sem=self.side_receive.at[kind, way - 2, part],
            device_id=self.device(way),
            device_id_type=pl.DeviceIdType.MESH,
        )

    def here(self, kind):
        return pltpu.make_async_copy(
            self.sources[kind],
            self.pads[kind].at[self.own, :, self.parts[0], :],
            self.local.at[kind],
        )

    def start(self):
        for kind in range(2):
            self.here(kind).start()
        for kind in range(2):
            for way in range(2):
                @pl.when(self.has(way))
                def _():
                    self.vertical(kind, way).start()
            for way in (2, 3):
                @pl.when(self.has(way))
                def _():
                    self.sideways(kind, way, 0).start()
        for pad in self.pads:
            for way in range(2):
                @pl.when(jnp.logical_not(self.has(way)))
                def _():
                    for slot in range(self.slots):
                        place = pad.at[slot, :, self.parts[1 + way], :]
                        place[...] = jnp.zeros(place.shape, pad.dtype)

            if self.columns > 2:
                for way in (2, 3):
                    @pl.when(jnp.logical_not(self.has(way)))
                    def _():
                        place = pad.at[0 if way == 2 else self.slots - 1]
                        place[...] = jnp.zeros(place.shape, pad.dtype)

    def finish(self):
        for kind in range(2):
            for came in range(2):
                @pl.when(self.has(came))
                def _():
                    self.vertical(kind, 1 - came).wait_recv()
                    for way in (2, 3):
                        @pl.when(self.has(way))
                        def _():
                            self.sideways(kind, way, 1 + came).start()
        for kind in range(2):
            self.here(kind).wait()
            for came in (2, 3):
                @pl.when(self.has(came))
                def _():
                    self.sideways(kind, 5 - came, 0).wait_recv()
                    for part in range(2):
                        @pl.when(self.has(part))
                        def _():
                            self.sideways(kind, 5 - came, 1 + part).wait_recv()

    def sent(self):
        for kind in range(2):
            for way in range(2):
                @pl.when(self.has(way))
                def _():
                    self.vertical(kind, way).wait_send()
            for way in (2, 3):
                @pl.when(self.has(way))
                def _():
                    self.sideways(kind, way, 0).wait_send()
                    for part in range(2):
                        @pl.when(self.has(part))
                        def _():
                            self.sideways(kind, way, 1 + part).wait_send()


def weigh(scores, allowed):
    scores = jnp.where(allowed, scores, -jnp.inf)
    raised = jnp.exp(scores - jnp.max(scores, axis=-1, keepdims=True))
    return (raised * (1.0 / jnp.sum(raised, axis=-1, keepdims=True))).astype(jnp.bfloat16)


def score(queries, keys):
    return lax.dot_general(
        queries, keys, (((1,), (1,)), ((), ())), preferred_element_type=jnp.float32
    ) * (1.0 / math.sqrt(HD))


def attend_kernel(
    stride, grid_columns, frames, side,
    query_ref, key_ref, value_ref, output_hbm,
    result_ref,
    key_pad, value_pad, spatial, mixed, held, total, local, send, receive, line_send, line_receive,
    halo_local, halo_send, halo_receive, side_send, side_receive,
):
    cube = Cube(stride)
    rows, columns = output_hbm.shape
    weight = Exchange(cube, held, send, receive, rows)
    load = pltpu.make_async_copy(output_hbm, weight.own, local)
    load.start()
    group_width = query_ref.shape[1]
    heads_here = group_width // HD
    tokens = query_ref.shape[0]

    def head_of(at):
        return pl.ds(pl.multiple_of(at * HD, HD), HD)

    line = Line(lambda group, at: mixed.at[group, :, head_of(at)], line_send, line_receive)
    halo = Halo(
        (key_ref, value_ref), (key_pad, value_pad), grid_columns, side,
        halo_local, halo_send, halo_receive, side_send, side_receive,
    )
    cube.barrier((line, halo))
    halo.start()
    load.wait()
    weight.start(2, 0, 1)

    area = side * side
    tall = side + 2 * WT
    window = tall * side
    keys_here = halo.slots * window
    tiles = side // WT
    query_at = lax.broadcasted_iota(jnp.int32, (area, keys_here), 0)
    key_at = lax.broadcasted_iota(jnp.int32, (area, keys_here), 1)
    key_row = halo.row * tiles - 1 + key_at % window // side // WT
    key_column = (halo.first_column() + key_at // window) * tiles + key_at % side // WT
    down = key_row - halo.row * tiles - query_at // side // WT
    right = key_column - halo.column * tiles - query_at % side // WT
    near = (down >= -1) & (down <= 1) & (right >= -1) & (right <= 1)
    near &= (key_row >= 0) & (key_row < DEV_ROWS * tiles)
    near &= (key_column >= 0) & (key_column < grid_columns * tiles)
    strip = 2 * area
    same = (
        lax.broadcasted_iota(jnp.int32, (strip, tokens), 0) % area
        == lax.broadcasted_iota(jnp.int32, (strip, tokens), 1) % area
    )

    halo.finish()

    def window_of(pad, frame, head):
        return jnp.concatenate([pad[slot, frame, :, head] for slot in range(halo.slots)], axis=0)

    @pl.loop(0, heads_here)
    def _(at):
        head = head_of(at)
        own_keys = key_ref[:, :, head].reshape(tokens, HD)
        scores = [
            score(query_ref[pl.ds(frame * area, area), head], window_of(key_pad, frame, head))
            for frame in range(frames)
        ]
        weights = [weigh(one, near) for one in scores]
        for frame in range(frames):
            spatial[pl.ds(frame * area, area), :] = jnp.dot(
                weights[frame], window_of(value_pad, frame, head), preferred_element_type=jnp.float32
            ).astype(jnp.bfloat16)
        for low in range(0, tokens, strip):
            over = weigh(score(query_ref[pl.ds(low, strip), head], own_keys), same)
            mixed[line.me, pl.ds(low, strip), head] = jnp.dot(
                over, spatial[...], preferred_element_type=jnp.float32
            ).astype(jnp.bfloat16)
        line.start(0, 0, at)
        line.start(1, 0, at)

    block = tokens // 2

    def multiply(group, first=False):
        @pl.loop(0, 2)
        def _(step):
            here = pl.ds(pl.multiple_of(step * block, block), block)
            product = jnp.dot(mixed[group, here, :], held[group], preferred_element_type=jnp.float32)
            if first:
                total[here, :] = product
            else:
                total[here, :] += product

    def relay(far):
        @pl.loop(0, heads_here)
        def _(at):
            line.relay(far, at)

    relay(0)
    weight.near()
    weight.arrived(2, 3, 4)
    if line.count > 2:
        relay(1)
    weight.far()
    weight.arrived(7, 8)
    multiply(line.me, True)
    for far in range(line.count - 1):
        if far > 1:
            relay(far)
        for side_at in range(2):
            @pl.when(line.holds(side_at, far + 1))
            def _():
                multiply(line.origin(side_at, far + 1))
    result_ref[...] = total[...].astype(result_ref.dtype)
    weight.sent()
    line.sent(heads_here)
    halo.sent()


def attend(queries, keys, values, output_weight, stride, grid_columns, frames, side):
    tokens, group_width = queries.shape
    rows, columns = output_weight.shape
    groups = lax.axis_size("head")
    pad = pltpu.VMEM(
        (min(3, grid_columns), frames, side * (side + 2 * WT), group_width), jnp.bfloat16
    )
    heads_here = group_width // HD
    vmem = pl.BlockSpec(memory_space=pltpu.VMEM)
    return pl.pallas_call(
        functools.partial(attend_kernel, stride, grid_columns, frames, side),
        out_shape=jax.ShapeDtypeStruct((tokens, columns), jnp.bfloat16),
        in_specs=[vmem] * 3 + [pl.BlockSpec(memory_space=pl.ANY)],
        out_specs=vmem,
        scratch_shapes=[
            pad,
            pad,
            pltpu.VMEM((tokens, HD), jnp.bfloat16),
            pltpu.VMEM((groups, tokens, group_width), jnp.bfloat16),
            pltpu.VMEM((CUBE // 2, 2 * rows, columns), output_weight.dtype),
            pltpu.VMEM((tokens, columns), jnp.float32),
            pltpu.SemaphoreType.DMA,
            pltpu.SemaphoreType.DMA((9,)),
            pltpu.SemaphoreType.DMA((9,)),
            pltpu.SemaphoreType.DMA((2, groups - 1, heads_here)),
            pltpu.SemaphoreType.DMA((2, groups - 1, heads_here)),
            pltpu.SemaphoreType.DMA((2,)),
            pltpu.SemaphoreType.DMA((2, 2)),
            pltpu.SemaphoreType.DMA((2, 2)),
            pltpu.SemaphoreType.DMA((2, 2, 3)),
            pltpu.SemaphoreType.DMA((2, 2, 3)),
        ],
        compiler_params=pltpu.CompilerParams(
            collective_id=1, has_side_effects=True, vmem_limit_bytes=60 * 1024 * 1024
        ),
        name="attend",
    )(queries, keys, values, output_weight)


def pregather(weight, stride):
    if stride == 1:
        return weight
    count = lax.axis_size("hw")
    groups = [list(range(first, first + stride)) for first in range(0, count, stride)]
    return lax.all_gather(weight, "hw", axis=0, tiled=True, axis_index_groups=groups)


def per_device(
    latents,
    query_weight,
    key_weight,
    value_weight,
    output_weight,
    query_gain,
    key_gain,
    frame_index,
    row_index,
    column_index,
):
    frames, side, width = (latents.shape[1], latents.shape[2], latents.shape[4])
    tokens = latents.reshape(frames * side * side, width)
    head_dim = HD
    full_width = HEADS * HD
    group_width = query_weight.shape[1]
    heads_here = group_width // head_dim
    grid_columns = lax.axis_size("hw") // DEV_ROWS
    place = lax.axis_index("hw")
    grid_row = place // grid_columns
    grid_column = place % grid_columns
    stride = lax.axis_size("hw") // CUBE
    query_lin, key_lin, values = project(
        tokens,
        *(pregather(w, stride) for w in (query_weight, key_weight, value_weight)),
        stride,
    )
    query_squares, key_squares = lax.psum(
        (jnp.sum(query_lin * query_lin, axis=1), jnp.sum(key_lin * key_lin, axis=1)), "head"
    )
    query_norm = query_lin * lax.rsqrt(query_squares / full_width + NORM_EPS)[:, None] * query_gain
    key_norm = key_lin * lax.rsqrt(key_squares / full_width + NORM_EPS)[:, None] * key_gain
    rows_here = lax.dynamic_slice_in_dim(row_index, grid_row * side, side)
    columns_here = lax.dynamic_slice_in_dim(column_index, grid_column * side, side)
    angle = rope_angles(frame_index, rows_here, columns_here, head_dim)
    cosine, sine = jnp.cos(angle), jnp.sin(angle)
    queries = rotate(query_norm, cosine, sine, heads_here, head_dim)
    keys = rotate(key_norm, cosine, sine, heads_here, head_dim)
    result = attend(
        queries,
        keys.reshape(frames, -1, group_width),
        values.reshape(frames, -1, group_width),
        pregather(output_weight, stride),
        stride,
        grid_columns,
        frames,
        side,
    )
    return result.reshape(1, frames, side, side, output_weight.shape[1])


def solution(mesh):
    placed = (
        P("hw", None, None, None, None),
        P("hw", "head"),
        P("hw", "head"),
        P("hw", "head"),
        P("hw", "head"),
        P("head"),
        P("head"),
        P(),
        P(),
        P(),
    )
    return jax.shard_map(
        per_device,
        mesh=mesh,
        in_specs=placed,
        out_specs=P("hw", None, None, None, "head"),
        check_vma=False,
    )
```

```python
import functools
import math

import jax
import jax.numpy as jnp
from jax import lax
from jax.experimental import pallas as pl
from jax.experimental.pallas import tpu as pltpu
from jax.sharding import PartitionSpec as P

HEADS = 20
HD = 128
WT = 4
DEV_ROWS = 4


NORM_EPS = 0.5


def freq_table(count):
    ratios = jnp.arange(count, dtype=jnp.float32) / count
    return jnp.float32(10000.0) ** (-ratios)


def rope_angles(frame_index, row_index, column_index, head_dim):
    side_pairs = head_dim // 6
    frame_pairs = head_dim // 2 - 2 * side_pairs

    def lanes(before, count, after):
        return jnp.repeat(jnp.pad(freq_table(count), (before, after)), 2)

    frame_part = frame_index.astype(jnp.float32)[:, None] * lanes(0, frame_pairs, 2 * side_pairs)
    row_part = row_index.astype(jnp.float32)[:, None] * lanes(frame_pairs, side_pairs, side_pairs)
    column_part = column_index.astype(jnp.float32)[:, None] * lanes(
        frame_pairs + side_pairs, side_pairs, 0
    )
    total = frame_part[:, None, None] + row_part[:, None] + column_part
    return total.reshape(-1, head_dim)


def rotate(features, cosine, sine, heads_here, head_dim):
    even = lax.broadcasted_iota(jnp.int32, cosine.shape, 1) % 2 == 0
    heads = []
    for head in range(heads_here):
        one = features[:, head * head_dim : (head + 1) * head_dim]
        turned = jnp.where(even, -jnp.roll(one, -1, axis=1), jnp.roll(one, 1, axis=1))
        heads.append((one * cosine + turned * sine).astype(jnp.bfloat16))
    return jnp.concatenate(heads, axis=1)


CUBE = 8


class Cube:
    def __init__(self, stride):
        me = lax.axis_index("hw")
        within = lax.rem(me, stride) if stride > 1 else 0
        place = lax.div(me, stride) if stride > 1 else me
        core = lax.rem(place, 2)
        x = lax.rem(lax.div(place, 2), 2)
        y = lax.div(place, 4)
        self.place = place
        self.other = [place + 1 - 2 * core, place + 2 - 4 * x, place + 4 - 8 * y]
        self.diagonal = place + 2 - 4 * x + 4 - 8 * y
        self.devices = [{"hw": other * stride + within} for other in self.other]
        self.chip = lax.div(place, 2)
        self.chips = [
            self.chip,
            self.chip + 1 - 2 * x,
            self.chip + 2 - 4 * y,
            self.chip + 3 - 2 * x - 4 * y,
        ]

    def barrier(self, line=None):
        semaphore = pltpu.get_barrier_semaphore()
        if line is not None:
            for peers in line:
                peers.greet(semaphore)
        for device in self.devices:
            pl.semaphore_signal(semaphore, inc=1, device_id=device, device_id_type=pl.DeviceIdType.MESH)
        if line is None:
            pl.semaphore_wait(semaphore, len(self.devices))
        else:
            count = sum((peers.number() for peers in line), len(self.devices))
            pl.semaphore_wait(semaphore, count)


class Exchange:
    def __init__(self, cube, held, send, receive, rows):
        core_place, x_place, y_place = cube.other
        half = rows // 2

        def part(place, low, size):
            start = pl.multiple_of(lax.rem(place, 2) * rows + low, 16)
            return held.at[lax.div(place, 2), pl.ds(start, size)]

        def copy(at, place, low, size, partner):
            ref = part(place, low, size)
            return pltpu.make_async_remote_copy(
                src_ref=ref,
                dst_ref=ref,
                send_sem=send.at[at],
                recv_sem=receive.at[at],
                device_id=cube.devices[partner],
                device_id_type=pl.DeviceIdType.MESH,
            )

        self.own = part(cube.place, 0, rows)
        self.copies = [
            copy(0, cube.place, 0, rows, 1),
            copy(1, cube.place, 0, rows, 2),
            copy(2, cube.place, 0, rows, 0),
            copy(3, x_place, 0, rows, 0),
            copy(4, y_place, 0, rows, 0),
            copy(5, x_place, 0, half, 2),
            copy(6, y_place, half, half, 1),
            copy(7, cube.diagonal, 0, half, 0),
            copy(8, cube.diagonal, half, half, 0),
        ]

    def start(self, *which):
        for at in which:
            self.copies[at].start()

    def arrived(self, *which):
        for at in which:
            self.copies[at].wait_recv()

    def near(self):
        self.arrived(0)
        self.start(5, 3)
        self.arrived(1)
        self.start(6, 4)

    def far(self):
        self.arrived(5)
        self.start(7)
        self.arrived(6)
        self.start(8)

    def sent(self):
        for one in self.copies:
            one.wait_send()


class Peers:
    def __init__(self, parts, send, receive):
        self.count = lax.axis_size("head")
        self.me = lax.axis_index("head")
        self.parts, self.send, self.receive = parts, send, receive

    def device(self, step):
        return {"head": lax.rem(self.me + step, self.count)}

    def greet(self, semaphore):
        for step in range(1, self.count):
            pl.semaphore_signal(
                semaphore,
                inc=1,
                device_id=self.device(step),
                device_id_type=pl.DeviceIdType.MESH,
            )

    def number(self):
        return self.count - 1

    def copy(self, step, group):
        ref = self.parts.at[group]
        return pltpu.make_async_remote_copy(
            src_ref=ref,
            dst_ref=ref,
            send_sem=self.send.at[step - 1],
            recv_sem=self.receive.at[step - 1],
            device_id=self.device(step),
            device_id_type=pl.DeviceIdType.MESH,
        )

    def start(self):
        for step in range(1, self.count):
            self.copy(step, self.me).start()

    def finish(self):
        for step in range(1, self.count):
            self.copy(step, lax.rem(self.me + self.count - step, self.count)).wait_recv()

    def sent(self):
        for step in range(1, self.count):
            self.copy(step, self.me).wait_send()


def project_kernel(
    stride, tokens_hbm, query_hbm, key_hbm, value_hbm,
    query_ref, key_ref, value_ref, squares_ref,
    tokens, held, value_sum, parts, local, send, receive, parts_send, parts_receive,
):
    cube = Cube(stride)
    rows = query_hbm.shape[0]
    depth = 2 * rows
    weights = [
        Exchange(cube, held.at[at], send.at[at], receive.at[at], rows) for at in range(3)
    ]
    loads = [
        pltpu.make_async_copy(source, weight.own, local.at[at])
        for at, (source, weight) in enumerate(
            zip((query_hbm, key_hbm, value_hbm), weights)
        )
    ]
    fetch = pltpu.make_async_copy(tokens_hbm, tokens, local.at[3])
    for load in loads:
        load.start()
    fetch.start()
    peers = Peers(parts, parts_send, parts_receive)
    cube.barrier((peers,))
    query, key, value = weights
    loads[0].wait()
    query.start(2, 0, 1)
    loads[1].wait()
    key.start(2, 0, 1)
    sums = [query_ref, key_ref, value_sum]
    block = tokens.shape[0] // 2

    def multiply(at, lane):
        chip = cube.chips[lane]

        @pl.loop(0, 2)
        def _(step):
            here = pl.ds(pl.multiple_of(step * block, block), block)
            product = jnp.dot(
                tokens[here, pl.ds(pl.multiple_of(chip * depth, 128), depth)],
                held[at, chip],
                preferred_element_type=jnp.float32,
            )
            if lane == 0:
                sums[at][here, :] = product
            else:
                sums[at][here, :] += product

    def near_multiply(at):
        weights[at].arrived(3)
        multiply(at, 1)
        weights[at].arrived(4)
        multiply(at, 2)

    def far_multiply(at):
        weights[at].arrived(7, 8)
        multiply(at, 3)

    loads[2].wait()
    fetch.wait()
    query.arrived(2)
    multiply(0, 0)
    key.arrived(2)
    multiply(1, 0)
    query.near()
    near_multiply(0)
    key.near()
    value.start(2, 0, 1)
    near_multiply(1)
    value.arrived(2)
    multiply(2, 0)
    query.far()
    far_multiply(0)
    key.far()
    far_multiply(1)
    for at in range(2):
        lin = sums[at][...]
        parts[peers.me, at] = lax.dot_general(
            jnp.ones((8, lin.shape[1]), jnp.float32),
            lin * lin,
            (((1,), (1,)), ((), ())),
            precision=lax.Precision.HIGHEST,
            preferred_element_type=jnp.float32,
        )
    peers.start()
    value.near()
    near_multiply(2)
    value.far()
    far_multiply(2)
    value_ref[...] = value_sum[...].astype(value_ref.dtype)
    peers.finish()
    squares_ref[...] = sum(parts[group] for group in range(peers.count))
    peers.sent()
    for weight in weights:
        weight.sent()


def project(tokens, query_weight, key_weight, value_weight, stride):
    count = tokens.shape[0]
    rows, width = query_weight.shape
    groups = lax.axis_size("head")
    anywhere = pl.BlockSpec(memory_space=pl.ANY)
    vmem = pl.BlockSpec(memory_space=pltpu.VMEM)
    return pl.pallas_call(
        functools.partial(project_kernel, stride),
        out_shape=(
            jax.ShapeDtypeStruct((count, width), jnp.float32),
            jax.ShapeDtypeStruct((count, width), jnp.float32),
            jax.ShapeDtypeStruct((count, width), jnp.bfloat16),
            jax.ShapeDtypeStruct((2, 8, count), jnp.float32),
        ),
        in_specs=[anywhere] * 4,
        out_specs=(vmem, vmem, vmem, vmem),
        scratch_shapes=[
            pltpu.VMEM(tokens.shape, tokens.dtype),
            pltpu.VMEM((3, CUBE // 2, 2 * rows, width), query_weight.dtype),
            pltpu.VMEM((count, width), jnp.float32),
            pltpu.VMEM((groups, 2, 8, count), jnp.float32),
            pltpu.SemaphoreType.DMA((4,)),
            pltpu.SemaphoreType.DMA((3, 9)),
            pltpu.SemaphoreType.DMA((3, 9)),
            pltpu.SemaphoreType.DMA((groups - 1,)),
            pltpu.SemaphoreType.DMA((groups - 1,)),
        ],
        compiler_params=pltpu.CompilerParams(
            collective_id=0, has_side_effects=True, vmem_limit_bytes=60 * 1024 * 1024
        ),
        name="project",
    )(tokens, query_weight, key_weight, value_weight)


class Line:
    def __init__(self, blocks, send, receive):
        self.count = lax.axis_size("head")
        self.me = lax.axis_index("head")
        self.blocks, self.send, self.receive = blocks, send, receive

    def neighbour(self, side):
        return self.me + 1 if side == 0 else self.me - 1

    def has(self, side):
        return self.me < self.count - 1 if side == 0 else self.me > 0

    def greet(self, semaphore):
        for side in range(2):
            @pl.when(self.has(side))
            def _():
                pl.semaphore_signal(
                    semaphore,
                    inc=1,
                    device_id={"head": self.neighbour(side)},
                    device_id_type=pl.DeviceIdType.MESH,
                )

    def number(self):
        return ones(self.me, self.count)

    def origin(self, side, far):
        return self.me - far if side == 0 else self.me + far

    def holds(self, side, far):
        return self.me >= far if side == 0 else self.me + far < self.count

    def copy(self, side, far, at, group):
        ref = self.blocks(group, at)
        return pltpu.make_async_remote_copy(
            src_ref=ref,
            dst_ref=ref,
            send_sem=self.send.at[side, far, at],
            recv_sem=self.receive.at[side, far, at],
            device_id={"head": self.neighbour(side)},
            device_id_type=pl.DeviceIdType.MESH,
        )

    def start(self, side, far, at):
        @pl.when(self.has(side) & self.holds(side, far))
        def _():
            self.copy(side, far, at, self.origin(side, far)).start()

    def relay(self, far, at):
        for side in range(2):
            @pl.when(self.holds(side, far + 1))
            def _():
                self.copy(side, far, at, self.origin(side, far + 1)).wait_recv()

            if far + 2 < self.count:
                self.start(side, far + 1, at)

    def sent(self, parts):
        for side in range(2):
            for far in range(self.count - 1):
                @pl.when(self.has(side) & self.holds(side, far))
                def _():
                    @pl.loop(0, parts)
                    def _(at):
                        self.copy(side, far, at, self.origin(side, far)).wait_send()


def ones(me, count):
    return 1 - lax.div(me + 1, count) + lax.div(me + count - 1, count)


class Halo:
    def __init__(self, sources, pads, grid_columns, side, local, send, receive, side_send, side_receive):
        place = lax.axis_index("hw")
        self.row, self.column = lax.div(place, grid_columns), lax.rem(place, grid_columns)
        self.place, self.columns = place, grid_columns
        self.sources, self.pads = sources, pads
        self.edge, self.body = WT * side, side * side
        self.slots = min(3, grid_columns)
        self.own = self.column if grid_columns == 2 else self.slots // 2
        self.local, self.send, self.receive = local, send, receive
        self.side_send, self.side_receive = side_send, side_receive
        self.parts = [
            pl.ds(self.edge, self.body),
            pl.ds(0, self.edge),
            pl.ds(self.edge + self.body, self.edge),
        ]

    def first_column(self):
        return 0 if self.columns == 2 else self.column - self.slots // 2

    def has(self, way):
        return [
            self.row > 0,
            self.row < DEV_ROWS - 1,
            self.column > 0,
            self.column < self.columns - 1,
        ][way]

    def device(self, way):
        step = [-self.columns, self.columns, -1, 1][way]
        return {"hw": self.place + step}

    def greet(self, semaphore):
        for way in range(4):
            @pl.when(self.has(way))
            def _():
                pl.semaphore_signal(
                    semaphore,
                    inc=1,
                    device_id=self.device(way),
                    device_id_type=pl.DeviceIdType.MESH,
                )

    def number(self):
        return ones(self.row, DEV_ROWS) + ones(self.column, self.columns)

    def vertical(self, kind, way):
        low = 0 if way == 0 else self.body - self.edge
        return pltpu.make_async_remote_copy(
            src_ref=self.sources[kind].at[:, pl.ds(low, self.edge), :],
            dst_ref=self.pads[kind].at[self.own, :, self.parts[2 - way], :],
            send_sem=self.send.at[kind, way],
            recv_sem=self.receive.at[kind, way],
            device_id=self.device(way),
            device_id_type=pl.DeviceIdType.MESH,
        )

    def sideways(self, kind, way, part):
        own = self.pads[kind].at[self.own, :, self.parts[part], :]
        if self.columns == 2:
            slot = self.own
        else:
            slot = self.slots - 1 if way == 2 else 0
        return pltpu.make_async_remote_copy(
            src_ref=self.sources[kind] if part == 0 else own,
            dst_ref=self.pads[kind].at[slot, :, self.parts[part], :],
            send_sem=self.side_send.at[kind, way - 2, part],
            recv_sem=self.side_receive.at[kind, way - 2, part],
            device_id=self.device(way),
            device_id_type=pl.DeviceIdType.MESH,
        )

    def here(self, kind):
        return pltpu.make_async_copy(
            self.sources[kind],
            self.pads[kind].at[self.own, :, self.parts[0], :],
            self.local.at[kind],
        )

    def start(self):
        for kind in range(2):
            self.here(kind).start()
        for kind in range(2):
            for way in range(2):
                @pl.when(self.has(way))
                def _():
                    self.vertical(kind, way).start()
            for way in (2, 3):
                @pl.when(self.has(way))
                def _():
                    self.sideways(kind, way, 0).start()
        for pad in self.pads:
            for way in range(2):
                @pl.when(jnp.logical_not(self.has(way)))
                def _():
                    for slot in range(self.slots):
                        place = pad.at[slot, :, self.parts[1 + way], :]
                        place[...] = jnp.zeros(place.shape, pad.dtype)

            if self.columns > 2:
                for way in (2, 3):
                    @pl.when(jnp.logical_not(self.has(way)))
                    def _():
                        place = pad.at[0 if way == 2 else self.slots - 1]
                        place[...] = jnp.zeros(place.shape, pad.dtype)

    def finish(self):
        for kind in range(2):
            for came in range(2):
                @pl.when(self.has(came))
                def _():
                    self.vertical(kind, 1 - came).wait_recv()
                    for way in (2, 3):
                        @pl.when(self.has(way))
                        def _():
                            self.sideways(kind, way, 1 + came).start()
        for kind in range(2):
            self.here(kind).wait()
            for came in (2, 3):
                @pl.when(self.has(came))
                def _():
                    self.sideways(kind, 5 - came, 0).wait_recv()
                    for part in range(2):
                        @pl.when(self.has(part))
                        def _():
                            self.sideways(kind, 5 - came, 1 + part).wait_recv()

    def sent(self):
        for kind in range(2):
            for way in range(2):
                @pl.when(self.has(way))
                def _():
                    self.vertical(kind, way).wait_send()
            for way in (2, 3):
                @pl.when(self.has(way))
                def _():
                    self.sideways(kind, way, 0).wait_send()
                    for part in range(2):
                        @pl.when(self.has(part))
                        def _():
                            self.sideways(kind, way, 1 + part).wait_send()


def weigh(scores, allowed):
    scores = jnp.where(allowed, scores, -jnp.inf)
    raised = jnp.exp(scores - jnp.max(scores, axis=-1, keepdims=True))
    return (raised * (1.0 / jnp.sum(raised, axis=-1, keepdims=True))).astype(jnp.bfloat16)


def score(queries, keys):
    return lax.dot_general(
        queries, keys, (((1,), (1,)), ((), ())), preferred_element_type=jnp.float32
    ) * (1.0 / math.sqrt(HD))


def attend_kernel(
    stride, grid_columns, frames, side,
    query_ref, key_ref, value_ref, output_hbm,
    result_ref,
    key_pad, value_pad, spatial, mixed, held, total, local, send, receive, line_send, line_receive,
    halo_local, halo_send, halo_receive, side_send, side_receive,
):
    cube = Cube(stride)
    rows, columns = output_hbm.shape
    weight = Exchange(cube, held, send, receive, rows)
    load = pltpu.make_async_copy(output_hbm, weight.own, local)
    load.start()
    group_width = query_ref.shape[1]
    heads_here = group_width // HD
    tokens = query_ref.shape[0]

    def head_of(at):
        return pl.ds(pl.multiple_of(at * HD, HD), HD)

    line = Line(lambda group, at: mixed.at[group, :, head_of(at)], line_send, line_receive)
    halo = Halo(
        (key_ref, value_ref), (key_pad, value_pad), grid_columns, side,
        halo_local, halo_send, halo_receive, side_send, side_receive,
    )
    cube.barrier((line, halo))
    halo.start()
    load.wait()

    area = side * side
    tall = side + 2 * WT
    window = tall * side
    keys_here = halo.slots * window
    tiles = side // WT
    query_at = lax.broadcasted_iota(jnp.int32, (area, keys_here), 0)
    key_at = lax.broadcasted_iota(jnp.int32, (area, keys_here), 1)
    key_row = halo.row * tiles - 1 + key_at % window // side // WT
    key_column = (halo.first_column() + key_at // window) * tiles + key_at % side // WT
    down = key_row - halo.row * tiles - query_at // side // WT
    right = key_column - halo.column * tiles - query_at % side // WT
    near = (down >= -1) & (down <= 1) & (right >= -1) & (right <= 1)
    near &= (key_row >= 0) & (key_row < DEV_ROWS * tiles)
    near &= (key_column >= 0) & (key_column < grid_columns * tiles)
    strip = 2 * area
    same = (
        lax.broadcasted_iota(jnp.int32, (strip, tokens), 0) % area
        == lax.broadcasted_iota(jnp.int32, (strip, tokens), 1) % area
    )

    halo.finish()
    weight.start(2, 0, 1)

    def window_of(pad, frame, head):
        return jnp.concatenate([pad[slot, frame, :, head] for slot in range(halo.slots)], axis=0)

    @pl.loop(0, heads_here)
    def _(at):
        head = head_of(at)
        own_keys = key_ref[:, :, head].reshape(tokens, HD)
        scores = [
            score(query_ref[pl.ds(frame * area, area), head], window_of(key_pad, frame, head))
            for frame in range(frames)
        ]
        weights = [weigh(one, near) for one in scores]
        for frame in range(frames):
            spatial[pl.ds(frame * area, area), :] = jnp.dot(
                weights[frame], window_of(value_pad, frame, head), preferred_element_type=jnp.float32
            ).astype(jnp.bfloat16)
        for low in range(0, tokens, strip):
            over = weigh(score(query_ref[pl.ds(low, strip), head], own_keys), same)
            mixed[line.me, pl.ds(low, strip), head] = jnp.dot(
                over, spatial[...], preferred_element_type=jnp.float32
            ).astype(jnp.bfloat16)
        line.start(0, 0, at)
        line.start(1, 0, at)

    block = tokens // 2

    def multiply(group, first=False):
        @pl.loop(0, 2)
        def _(step):
            here = pl.ds(pl.multiple_of(step * block, block), block)
            product = jnp.dot(mixed[group, here, :], held[group], preferred_element_type=jnp.float32)
            if first:
                total[here, :] = product
            else:
                total[here, :] += product

    def relay(far):
        @pl.loop(0, heads_here)
        def _(at):
            line.relay(far, at)

    relay(0)
    weight.near()
    weight.arrived(2, 3, 4)
    if line.count > 2:
        relay(1)
    weight.far()
    weight.arrived(7, 8)
    multiply(line.me, True)
    for far in range(line.count - 1):
        if far > 1:
            relay(far)
        for side_at in range(2):
            @pl.when(line.holds(side_at, far + 1))
            def _():
                multiply(line.origin(side_at, far + 1))
    result_ref[...] = total[...].astype(result_ref.dtype)
    weight.sent()
    line.sent(heads_here)
    halo.sent()


def attend(queries, keys, values, output_weight, stride, grid_columns, frames, side):
    tokens, group_width = queries.shape
    rows, columns = output_weight.shape
    groups = lax.axis_size("head")
    pad = pltpu.VMEM(
        (min(3, grid_columns), frames, side * (side + 2 * WT), group_width), jnp.bfloat16
    )
    heads_here = group_width // HD
    vmem = pl.BlockSpec(memory_space=pltpu.VMEM)
    return pl.pallas_call(
        functools.partial(attend_kernel, stride, grid_columns, frames, side),
        out_shape=jax.ShapeDtypeStruct((tokens, columns), jnp.bfloat16),
        in_specs=[vmem] * 3 + [pl.BlockSpec(memory_space=pl.ANY)],
        out_specs=vmem,
        scratch_shapes=[
            pad,
            pad,
            pltpu.VMEM((tokens, HD), jnp.bfloat16),
            pltpu.VMEM((groups, tokens, group_width), jnp.bfloat16),
            pltpu.VMEM((CUBE // 2, 2 * rows, columns), output_weight.dtype),
            pltpu.VMEM((tokens, columns), jnp.float32),
            pltpu.SemaphoreType.DMA,
            pltpu.SemaphoreType.DMA((9,)),
            pltpu.SemaphoreType.DMA((9,)),
            pltpu.SemaphoreType.DMA((2, groups - 1, heads_here)),
            pltpu.SemaphoreType.DMA((2, groups - 1, heads_here)),
            pltpu.SemaphoreType.DMA((2,)),
            pltpu.SemaphoreType.DMA((2, 2)),
            pltpu.SemaphoreType.DMA((2, 2)),
            pltpu.SemaphoreType.DMA((2, 2, 3)),
            pltpu.SemaphoreType.DMA((2, 2, 3)),
        ],
        compiler_params=pltpu.CompilerParams(
            collective_id=1, has_side_effects=True, vmem_limit_bytes=60 * 1024 * 1024
        ),
        name="attend",
    )(queries, keys, values, output_weight)


def pregather(weight, stride):
    if stride == 1:
        return weight
    count = lax.axis_size("hw")
    groups = [list(range(first, first + stride)) for first in range(0, count, stride)]
    return lax.all_gather(weight, "hw", axis=0, tiled=True, axis_index_groups=groups)


def per_device(
    latents,
    query_weight,
    key_weight,
    value_weight,
    output_weight,
    query_gain,
    key_gain,
    frame_index,
    row_index,
    column_index,
):
    frames, side, width = (latents.shape[1], latents.shape[2], latents.shape[4])
    tokens = latents.reshape(frames * side * side, width)
    head_dim = HD
    full_width = HEADS * HD
    group_width = query_weight.shape[1]
    heads_here = group_width // head_dim
    grid_columns = lax.axis_size("hw") // DEV_ROWS
    place = lax.axis_index("hw")
    grid_row = place // grid_columns
    grid_column = place % grid_columns
    stride = lax.axis_size("hw") // CUBE
    query_lin, key_lin, values, squares = project(
        tokens,
        *(pregather(w, stride) for w in (query_weight, key_weight, value_weight)),
        stride,
    )
    query_squares, key_squares = squares[0, 0], squares[1, 0]
    query_norm = query_lin * lax.rsqrt(query_squares / full_width + NORM_EPS)[:, None] * query_gain
    key_norm = key_lin * lax.rsqrt(key_squares / full_width + NORM_EPS)[:, None] * key_gain
    rows_here = lax.dynamic_slice_in_dim(row_index, grid_row * side, side)
    columns_here = lax.dynamic_slice_in_dim(column_index, grid_column * side, side)
    angle = rope_angles(frame_index, rows_here, columns_here, head_dim)
    cosine, sine = jnp.cos(angle), jnp.sin(angle)
    queries = rotate(query_norm, cosine, sine, heads_here, head_dim)
    keys = rotate(key_norm, cosine, sine, heads_here, head_dim)
    result = attend(
        queries,
        keys.reshape(frames, -1, group_width),
        values.reshape(frames, -1, group_width),
        pregather(output_weight, stride),
        stride,
        grid_columns,
        frames,
        side,
    )
    return result.reshape(1, frames, side, side, output_weight.shape[1])


def solution(mesh):
    placed = (
        P("hw", None, None, None, None),
        P("hw", "head"),
        P("hw", "head"),
        P("hw", "head"),
        P("hw", "head"),
        P("head"),
        P("head"),
        P(),
        P(),
        P(),
    )
    return jax.shard_map(
        per_device,
        mesh=mesh,
        in_specs=placed,
        out_specs=P("hw", None, None, None, "head"),
        check_vma=False,
    )
```
